16 devices in a mesh: dp: 1, tp: 16 (over x, y, z, core).
Axes of the slice: x: 2, y: 2, z: 2, core: 2. Of those that a mesh axis runs over, the one named last changes fastest.
Arguments:
- x: bfloat16 [1536, 12288], P(('dp', 'tp'))
- w: bfloat16 [12288, 32768], P(None, 'tp')
- label: int32 [1536], P(('dp', 'tp'))
Outputs:
- output 1: float32 [1536], P(('dp', 'tp'))
- output 2: bfloat16 [1536, 12288], P(('dp', 'tp'))
- output 3: bfloat16 [12288, 32768], P('dp', 'tp')
All inputs are finite; a program needn't handle non-finite values.
Results may differ from the reference program's by a relative error of at most 0.012.
Values are sent between devices in bfloat16 or wider.
A program may use at most 2 GiB of HBM per device.

```python
import jax
import jax.numpy as jnp

ROWS = 1536
D = 12288
VOCAB = 32768


def setup_inputs(seed: int = 0, part: int = 0) -> dict:
    kx, kw, kl = jax.random.split(jax.random.key(seed), 3)
    kx, kl = (jax.random.fold_in(k, part) for k in (kx, kl))
    return {
        "x": jax.random.normal(kx, (ROWS, D), jnp.float32).astype(jnp.bfloat16),
        "w": (jax.random.normal(kw, (D, VOCAB), jnp.float32) * (4.0 / D) ** 0.5).astype(jnp.bfloat16),
        "label": jax.random.randint(kl, (ROWS,), 0, VOCAB, jnp.int32),
    }


def reference(x, w, label):
    logits = jnp.dot(x, w, preferred_element_type=jnp.float32)
    top = jnp.max(logits, -1, keepdims=True)
    e = jnp.exp(logits - top)
    total = jnp.sum(e, -1, keepdims=True)
    hit = label[:, None] == jnp.arange(VOCAB, dtype=jnp.int32)[None, :]
    loss = jnp.log(total[:, 0]) + top[:, 0] - jnp.sum(jnp.where(hit, logits, 0.0), -1)
    by_logits = (e / total - hit.astype(jnp.float32)).astype(jnp.bfloat16)
    by_x = jnp.dot(by_logits, w.T, preferred_element_type=jnp.float32).astype(jnp.bfloat16)
    by_w = jnp.dot(x.T, by_logits, preferred_element_type=jnp.float32).astype(jnp.bfloat16)
    return loss, by_x, by_w
```

```python
import functools

import jax
import jax.numpy as jnp
from jax import lax
from jax.experimental import pallas as pl
from jax.experimental.pallas import tpu as pltpu
from jax.sharding import PartitionSpec as P

MESH = pl.DeviceIdType.MESH
F32, BF16 = jnp.float32, jnp.bfloat16


def _where_am_i():
    me = lax.axis_index("tp")
    x, y, z, c = me // 8, (me // 4) % 2, (me // 2) % 2, me % 2
    return me, 8 - 16 * x, 4 - 8 * y, 2 - 4 * z, 1 - 2 * c


def _greet(peers):
    barrier = pltpu.get_barrier_semaphore()
    for p in peers:
        pl.semaphore_signal(barrier, inc=1, device_id={"tp": p}, device_id_type=MESH)
    pl.semaphore_wait(barrier, len(peers))


def _send(src, dst, send_sem, recv_sem, peer):
    return pltpu.make_async_remote_copy(
        src_ref=src, dst_ref=dst, send_sem=send_sem, recv_sem=recv_sem,
        device_id={"tp": peer}, device_id_type=MESH)


GATHER_SLOTS = 12


def gather_logits(td, x_hbm, lab_ref, w_hbm, xf_hbm, g_hbm, loss_ref,
                  xg, acc, wb, labs, cols, stat, s_out, s_in, gst,
                  send, recv, own_sem, back_sem, w_sem, lab_send, lab_recv, st_send, st_recv, g_sem):
    me, sx, sy, sz, sc = _where_am_i()
    rows, depth = x_hbm.shape
    n = depth // td
    third = rows // 3
    vocab = acc.shape[1]
    core = me % 2
    px, py, pz, pc = me + sx, me + sy, me + sz, me + sc
    _greet((px, py, pz, pc))

    def at(k):
        return pl.ds(pl.multiple_of(k * td, td), td)

    def block(k, dev):
        return xg.at[k % GATHER_SLOTS, dev // 2, dev % 2]

    def copies(k):
        s = k % GATHER_SLOTS

        def copy(i):
            if i < 3:
                src, dst, p = x_hbm.at[:, at(k)], block(k, me), (px, py, pz)[i]
            elif i < 6:
                dev, p = ((px, py), (py, pz), (pz, px))[i - 3]
                src = dst = block(k, dev)
            elif i < 9:
                dev, p = ((px + sy, pz), (py + sz, px), (pz + sx, py))[i - 6]
                src = dst = block(k, dev).at[pl.ds((i - 6) * third, third)]
            else:
                p = pc
                src = dst = xg.at[s, :, core]
            return _send(src, dst, send.at[i, s], recv.at[i, s], p)

        return copy

    def own_copy(k):
        return pltpu.make_async_copy(x_hbm.at[:, at(k)], block(k, me), own_sem.at[k % GATHER_SLOTS])

    def back_copy(k):
        s = k % GATHER_SLOTS
        return pltpu.make_async_copy(xg.at[s], xf_hbm.at[:, :, :, at(k)], back_sem.at[s])

    def w_copy(k):
        rows_k = pl.ds(pl.multiple_of(k * td, td), td)
        return pltpu.make_async_copy(w_hbm.at[rows_k, :], wb.at[k % 2], w_sem.at[k % 2])

    labs[me] = lab_ref[...]

    def lab_copy(i):
        size = 1 << i
        p = (pc, pz, py, px)[i]
        part = labs.at[pl.ds((me // size) * size, size)]
        return _send(part, part, lab_send.at[i], lab_recv.at[i], p)

    w_copy(0).start()
    acc[...] = jnp.zeros_like(acc)

    def step(t, _):
        for i in range(5):
            @pl.when(t == 3 * i + 2)
            def _():
                if i > 0:
                    lab_copy(i - 1).wait()
                if i < 4:
                    lab_copy(i).start()

        k4 = t - 6

        @pl.when((k4 >= 0) & (k4 < n))
        def _():
            cs = copies(k4)
            for i in range(6, 9):
                cs(i).wait_recv()
            own_copy(k4).wait()
            cs(9).start()

        k3 = t - 4

        @pl.when((k3 >= 0) & (k3 < n))
        def _():
            cs = copies(k3)
            for i in range(3, 6):
                cs(i).wait_recv()
            for i in range(6, 9):
                cs(i).start()

        k2 = t - 2

        @pl.when((k2 >= 0) & (k2 < n))
        def _():
            cs = copies(k2)
            for i in range(3):
                cs(i).wait_recv()
            for i in range(3, 6):
                cs(i).start()

        @pl.when(t < n)
        def _():
            cs = copies(t)
            for i in range(3):
                cs(i).start()
            own_copy(t).start()

        k5 = t - 8

        @pl.when((k5 >= 0) & (k5 < n))
        def _():
            cs = copies(k5)
            cs(9).wait_recv()
            w_copy(k5).wait()

            @pl.when(k5 + 1 < n)
            def _():
                w_copy(k5 + 1).start()

            @pl.when(k5 > 0)
            def _():
                back_copy(k5 - 1).wait()

            back_copy(k5).start()
            for i in range(10):
                cs(i).wait_send()
            s, b = k5 % GATHER_SLOTS, k5 % 2
            width = min(512, vocab)

            def part(j, _):
                c = pl.ds(pl.multiple_of(j * width, width), width)
                lhs = xg[s].reshape(16 * rows, td)
                acc[:, c] += jnp.dot(lhs, wb[b, :, c], preferred_element_type=F32)
                return 0

            lax.fori_loop(0, vocab // width, part, 0)

        return 0

    lax.fori_loop(0, max(n + 8, 16), step, 0)
    back_copy(n - 1).wait()

    lane = lax.broadcasted_iota(jnp.int32, (rows, 128), 1)
    column = lax.broadcasted_iota(jnp.int32, (rows, vocab), 1)

    def spread(row):
        return jnp.transpose(jnp.broadcast_to(row, (128, 128)))[:rows]

    def local(d, _):
        z = acc[pl.ds(pl.multiple_of(d * rows, rows), rows), :]
        lab = spread(labs[d][:1]) - me * vocab
        cols[pl.ds(pl.multiple_of(d * rows, rows), rows), :] = lab
        m = jnp.max(z, 1, keepdims=True)
        total = jnp.sum(jnp.exp(z - m), 1, keepdims=True)
        right = jnp.sum(jnp.where(column == lab[:, :1], z, 0.0), 1, keepdims=True)
        t = jnp.where(lane == 0, m, jnp.where(lane == 1, total, right))
        t = jnp.transpose(jnp.concatenate([t, jnp.zeros((128 - rows, 128), F32)], 0))
        for i in range(3):
            stat[i, pl.ds(d, 1), :] = t[i:i + 1]
        return 0

    lax.fori_loop(0, 16, local, 0)
    m, total, right = stat[0], stat[1], stat[2]
    for i, p in enumerate((pc, pz, py, px)):
        s_out[i, 0], s_out[i, 1], s_out[i, 2] = m, total, right
        cp = _send(s_out.at[i], s_in.at[i], st_send.at[i], st_recv.at[i], p)
        cp.start()
        cp.wait()
        m2, total2, right2 = s_in[i, 0], s_in[i, 1], s_in[i, 2]
        top = jnp.maximum(m, m2)
        total = total * jnp.exp(m - top) + total2 * jnp.exp(m2 - top)
        m, right = top, right + right2
    lse = jnp.log(total) + m
    loss_ref[...] = lse - right
    stat[0] = lse

    def g_copy(d):
        return pltpu.make_async_copy(gst.at[pl.ds(pl.multiple_of(d * rows, rows), rows)], g_hbm.at[d // 2, d % 2], g_sem.at[d])

    def grad(d, _):
        r = pl.ds(pl.multiple_of(d * rows, rows), rows)
        l = spread(stat[0, pl.ds(d, 1), :])
        hit = column == cols[r, :][:, :1]
        gst[r, :] = (jnp.exp(acc[r, :] - l[:, :1]) - hit.astype(F32)).astype(BF16)
        g_copy(d).start()
        return 0

    lax.fori_loop(0, 16, grad, 0)
    lax.fori_loop(0, 16, lambda d, _: (g_copy(d).wait(), 0)[1], 0)


def call_gather_logits(x, lab, w, td):
    rows, depth = x.shape
    vocab = w.shape[1]
    s = GATHER_SLOTS
    anywhere, vmem = pl.BlockSpec(memory_space=pl.ANY), pl.BlockSpec(memory_space=pltpu.VMEM)
    return pl.pallas_call(
        functools.partial(gather_logits, td),
        out_shape=(
            jax.ShapeDtypeStruct((8, 2, rows, depth), BF16),
            jax.ShapeDtypeStruct((8, 2, rows, vocab), BF16),
            jax.ShapeDtypeStruct((16, 128), F32),
        ),
        in_specs=[anywhere, vmem, anywhere],
        out_specs=(anywhere, anywhere, vmem),
        scratch_shapes=[
            pltpu.VMEM((s, 8, 2, rows, td), BF16),
            pltpu.VMEM((16 * rows, vocab), F32),
            pltpu.VMEM((2, td, vocab), BF16),
            pltpu.VMEM((16, 8, 128), jnp.int32),
            pltpu.VMEM((16 * rows, 128), jnp.int32),
            pltpu.VMEM((3, 16, 128), F32),
            pltpu.VMEM((4, 3, 16, 128), F32),
            pltpu.VMEM((4, 3, 16, 128), F32),
            pltpu.VMEM((16 * rows, vocab), BF16),
            pltpu.SemaphoreType.DMA((10, s)),
            pltpu.SemaphoreType.DMA((10, s)),
            pltpu.SemaphoreType.DMA((s,)),
            pltpu.SemaphoreType.DMA((s,)),
            pltpu.SemaphoreType.DMA((2,)),
            pltpu.SemaphoreType.DMA((4,)),
            pltpu.SemaphoreType.DMA((4,)),
            pltpu.SemaphoreType.DMA((4,)),
            pltpu.SemaphoreType.DMA((4,)),
            pltpu.SemaphoreType.DMA((16,)),
        ],
        compiler_params=pltpu.CompilerParams(
            collective_id=0, has_side_effects=True, vmem_limit_bytes=60 << 20),
        cost_estimate=pl.CostEstimate(flops=2 * 16 * rows * depth * vocab, bytes_accessed=depth * vocab * 2, transcendentals=0),
        name="gather_logits",
    )(x, lab, w)


SLOTS = 10


def states_grad(td, g_hbm, w_hbm, out_ref, gv, wb, f, s0, r0, s1, r1, s2, r2, s3, r3, g_sem, w_sem, send, recv):
    me, sx, sy, sz, sc = _where_am_i()
    rows = g_hbm.shape[2]
    depth, vocab = w_hbm.shape
    n = depth // td
    third = rows // 3
    core = me % 2
    px, py, pz, pc = me + sx, me + sy, me + sz, me + sc
    chip = me // 2
    cx, cy, cz = sx // 2, sy // 2, sz // 2

    for h, c in enumerate((core, 1 - core)):
        pltpu.make_async_copy(g_hbm.at[:, c], gv.at[h], g_sem.at[h]).start()

    def w_copy(k):
        rows_k = pl.ds(pl.multiple_of(k * td, td), td)
        return pltpu.make_async_copy(w_hbm.at[rows_k, :], wb.at[k % 2], w_sem.at[k % 2])

    w_copy(0).start()
    _greet((px, py, pz, pc))

    def copies(k):
        s = k % SLOTS

        def copy(i):
            if i == 0:
                src, dst, p = s0.at[s], r0.at[s], pc
            elif i < 4:
                src, dst, p = s1.at[s, pl.ds((i - 1) * third, third)], r1.at[s, i - 1], (pz, px, py)[i - 1]
            elif i < 7:
                src, dst, p = s2.at[s, i - 4], r2.at[s, i - 4], (py, pz, px)[i - 4]
            else:
                src, dst, p = s3.at[s, i - 7], r3.at[s, i - 7], (px, py, pz)[i - 7]
            return _send(src, dst, send.at[i, s], recv.at[i, s], p)

        return copy

    def both(s, dest):
        return f[s, dest] + r0[s, dest].astype(F32)

    for h, c in enumerate((core, 1 - core)):
        pltpu.make_async_copy(g_hbm.at[:, c], gv.at[h], g_sem.at[h]).wait()

    def step(t, _):
        ke = t - 7

        @pl.when((ke >= 0) & (ke < n))
        def _():
            s = ke % SLOTS
            cs = copies(ke)
            for i in range(7, 10):
                cs(i).wait_recv()
            total = both(s, chip) + r3[s, 0].astype(F32) + r3[s, 1].astype(F32) + r3[s, 2].astype(F32)
            out_ref[:, pl.ds(pl.multiple_of(ke * td, td), td)] = total.astype(BF16)
            for i in range(10):
                cs(i).wait_send()

        kd = t - 5

        @pl.when((kd >= 0) & (kd < n))
        def _():
            s = kd % SLOTS
            cs = copies(kd)
            for i, dest in enumerate((chip + cx, chip + cy, chip + cz)):
                cs(4 + i).wait_recv()
                s3[s, i] = (both(s, dest) + r2[s, i].astype(F32)).astype(BF16)
                cs(7 + i).start()

        kc = t - 3

        @pl.when((kc >= 0) & (kc < n))
        def _():
            s = kc % SLOTS
            cs = copies(kc)
            for i, dest in enumerate((chip + cx + cy, chip + cy + cz, chip + cz + cx)):
                cs(1 + i).wait_recv()
                total = both(s, dest)
                a, b = i * third, (i + 1) * third
                middle = total[a:b] + r1[s, i].astype(F32)
                if i > 0:
                    s2[s, i, :a] = total[:a].astype(BF16)
                s2[s, i, a:b] = middle.astype(BF16)
                if i < 2:
                    s2[s, i, b:] = total[b:].astype(BF16)
                cs(4 + i).start()

        kb = t - 1

        @pl.when((kb >= 0) & (kb < n))
        def _():
            s = kb % SLOTS
            cs = copies(kb)
            cs(0).wait_recv()
            s1[s] = both(s, chip + cx + cy + cz).astype(BF16)
            for i in range(3):
                cs(1 + i).start()

        @pl.when(t < n)
        def _():
            s, b = t % SLOTS, t % 2
            w_copy(t).wait()

            @pl.when(t + 1 < n)
            def _():
                w_copy(t + 1).start()

            def term(h):
                lhs = gv[h].reshape(8 * rows, vocab)
                return lax.dot_general(lhs, wb[b], (((1,), (1,)), ((), ())), preferred_element_type=F32)

            s0[s] = term(1).astype(BF16).reshape(8, rows, td)
            copies(t)(0).start()
            f[s] = term(0).reshape(8, rows, td)

        return 0

    lax.fori_loop(0, n + 7, step, 0)


def call_states_grad(g, w, td):
    rows, vocab = g.shape[2:]
    depth = w.shape[0]
    s = SLOTS
    anywhere, vmem = pl.BlockSpec(memory_space=pl.ANY), pl.BlockSpec(memory_space=pltpu.VMEM)
    blocks = lambda *shape, dtype=BF16: pltpu.VMEM((*shape, td), dtype)
    return pl.pallas_call(
        functools.partial(states_grad, td),
        out_shape=jax.ShapeDtypeStruct((rows, depth), BF16),
        in_specs=[anywhere, anywhere],
        out_specs=vmem,
        scratch_shapes=[
            pltpu.VMEM((2, 8, rows, vocab), BF16),
            pltpu.VMEM((2, td, vocab), BF16),
            blocks(s, 8, rows, dtype=F32),
            blocks(s, 8, rows),
            blocks(s, 8, rows),
            blocks(s, rows),
            blocks(s, 3, rows // 3),
            blocks(s, 3, rows),
            blocks(s, 3, rows),
            blocks(s, 3, rows),
            blocks(s, 3, rows),
            pltpu.SemaphoreType.DMA((2,)),
            pltpu.SemaphoreType.DMA((2,)),
            pltpu.SemaphoreType.DMA((10, s)),
            pltpu.SemaphoreType.DMA((10, s)),
        ],
        compiler_params=pltpu.CompilerParams(
            collective_id=1, has_side_effects=True, vmem_limit_bytes=67043328),
        cost_estimate=pl.CostEstimate(flops=2 * 16 * rows * depth * vocab, bytes_accessed=depth * vocab * 2, transcendentals=0),
        name="states_grad",
    )(g, w)


def matrix_grad(x_ref, g_ref, out_ref):
    vocab = out_ref.shape[1]
    width = min(512, vocab)

    def part(j, _):
        c = pl.ds(pl.multiple_of(j * width, width), width)
        out_ref[:, c] = lax.dot_general(
            x_ref[...], g_ref[:, c], (((0,), (0,)), ((), ())), preferred_element_type=F32).astype(BF16)
        return 0

    lax.fori_loop(0, vocab // width, part, 0)


def call_matrix_grad(x, g, tile):
    rows, depth = x.shape
    vocab = g.shape[1]
    return pl.pallas_call(
        matrix_grad,
        grid=(depth // tile,),
        out_shape=jax.ShapeDtypeStruct((depth, vocab), BF16),
        in_specs=[pl.BlockSpec((rows, tile), lambda i: (0, i)), pl.BlockSpec((rows, vocab), lambda i: (0, 0))],
        out_specs=pl.BlockSpec((tile, vocab), lambda i: (i, 0)),
        compiler_params=pltpu.CompilerParams(vmem_limit_bytes=48 << 20),
        cost_estimate=pl.CostEstimate(flops=2 * rows * depth * vocab, bytes_accessed=2 * depth * (rows + vocab), transcendentals=0),
        name="matrix_grad",
    )(x, g)


def solution(mesh):
    def step(x, w, label):
        rows, depth = x.shape
        vocab = w.shape[1]
        td = 512 if depth % 512 == 0 and depth > 4096 else 128
        me = lax.axis_index("tp")
        lab = jnp.pad(label[None, :], ((0, 7), (0, 128 - rows)))
        xf, g, loss = call_gather_logits(x, lab, w, td)
        by_x = call_states_grad(g, w, td)
        by_w = call_matrix_grad(xf.reshape(16 * rows, depth), g.reshape(16 * rows, vocab), min(1024, depth))
        return lax.dynamic_slice_in_dim(loss[:, :rows], me, 1)[0], by_x, by_w

    return jax.shard_map(
        step,
        mesh=mesh,
        in_specs=(P(("dp", "tp"), None), P(None, "tp"), P(("dp", "tp"))),
        out_specs=(P(("dp", "tp")), P(("dp", "tp"), None), P("dp", "tp")),
        check_vma=False,
    )
```

```python
import functools

import jax
import jax.numpy as jnp
from jax import lax
from jax.experimental import pallas as pl
from jax.experimental.pallas import tpu as pltpu
from jax.sharding import PartitionSpec as P

MESH = pl.DeviceIdType.MESH
F32, BF16 = jnp.float32, jnp.bfloat16


def _where_am_i():
    me = lax.axis_index("tp")
    x, y, z, c = me // 8, (me // 4) % 2, (me // 2) % 2, me % 2
    return me, 8 - 16 * x, 4 - 8 * y, 2 - 4 * z, 1 - 2 * c


def _greet(peers):
    barrier = pltpu.get_barrier_semaphore()
    for p in peers:
        pl.semaphore_signal(barrier, inc=1, device_id={"tp": p}, device_id_type=MESH)
    pl.semaphore_wait(barrier, len(peers))


def _send(src, dst, send_sem, recv_sem, peer):
    return pltpu.make_async_remote_copy(
        src_ref=src, dst_ref=dst, send_sem=send_sem, recv_sem=recv_sem,
        device_id={"tp": peer}, device_id_type=MESH)


GATHER_SLOTS = 12


def gather_logits(td, x_hbm, lab_ref, w_hbm, xf_hbm, g_hbm, loss_ref,
                  xg, acc, wb, labs, cols, stat, scale, s_out, s_in, gst,
                  send, recv, own_sem, back_sem, w_sem, lab_send, lab_recv, st_send, st_recv, g_sem):
    me, sx, sy, sz, sc = _where_am_i()
    rows, depth = x_hbm.shape
    n = depth // td
    third = rows // 3
    vocab = acc.shape[1]
    core = me % 2
    px, py, pz, pc = me + sx, me + sy, me + sz, me + sc
    far = (px, py, pz, px + sy, py + sz, pz + sx, px + sy + sz)
    _greet((*far, pc))

    def at(k):
        return pl.ds(pl.multiple_of(k * td, td), td)

    def block(k, dev):
        return xg.at[k % GATHER_SLOTS, dev // 2, dev % 2]

    def copies(k):
        s = k % GATHER_SLOTS

        def copy(i):
            if i < 3:
                src, dst, p = x_hbm.at[:, at(k)], block(k, me), (px, py, pz)[i]
            elif i < 6:
                dev, p = ((px, py), (py, pz), (pz, px))[i - 3]
                src = dst = block(k, dev)
            elif i < 9:
                dev, p = ((px + sy, pz), (py + sz, px), (pz + sx, py))[i - 6]
                src = dst = block(k, dev).at[pl.ds((i - 6) * third, third)]
            else:
                p = pc
                src = dst = xg.at[s, :, core]
            return _send(src, dst, send.at[i, s], recv.at[i, s], p)

        return copy

    def own_copy(k):
        return pltpu.make_async_copy(x_hbm.at[:, at(k)], block(k, me), own_sem.at[k % GATHER_SLOTS])

    def back_copy(k):
        s = k % GATHER_SLOTS
        return pltpu.make_async_copy(xg.at[s], xf_hbm.at[:, :, :, at(k)], back_sem.at[s])

    def w_copy(k):
        rows_k = pl.ds(pl.multiple_of(k * td, td), td)
        return pltpu.make_async_copy(w_hbm.at[rows_k, :], wb.at[k % 2], w_sem.at[k % 2])

    labs[me] = lab_ref[...]

    def lab_copy(i):
        size = 1 << i
        p = (pc, pz, py, px)[i]
        part = labs.at[pl.ds((me // size) * size, size)]
        return _send(part, part, lab_send.at[i], lab_recv.at[i], p)

    w_copy(0).start()
    acc[...] = jnp.zeros_like(acc)

    def step(t, _):
        for i in range(5):
            @pl.when(t == 3 * i + 2)
            def _():
                if i > 0:
                    lab_copy(i - 1).wait()
                if i < 4:
                    lab_copy(i).start()

        k4 = t - 5

        @pl.when((k4 >= 0) & (k4 < n))
        def _():
            cs = copies(k4)
            for i in range(6, 9):
                cs(i).wait_recv()
            own_copy(k4).wait()
            cs(9).start()

        k3 = t - 4

        @pl.when((k3 >= 0) & (k3 < n))
        def _():
            cs = copies(k3)
            for i in range(3, 6):
                cs(i).wait_recv()
            for i in range(6, 9):
                cs(i).start()

        k2 = t - 2

        @pl.when((k2 >= 0) & (k2 < n))
        def _():
            cs = copies(k2)
            for i in range(3):
                cs(i).wait_recv()
            for i in range(3, 6):
                cs(i).start()

        @pl.when(t < n)
        def _():
            cs = copies(t)
            for i in range(3):
                cs(i).start()
            own_copy(t).start()

        k5 = t - 6

        @pl.when((k5 >= 0) & (k5 < n))
        def _():
            cs = copies(k5)
            cs(9).wait_recv()
            w_copy(k5).wait()

            @pl.when(k5 + 1 < n)
            def _():
                w_copy(k5 + 1).start()

            @pl.when(k5 > 0)
            def _():
                back_copy(k5 - 1).wait()

            back_copy(k5).start()
            for i in range(10):
                cs(i).wait_send()
            lhs = xg[k5 % GATHER_SLOTS].reshape(16 * rows, td)
            acc[...] += jnp.dot(lhs, wb[k5 % 2], preferred_element_type=F32)

        return 0

    lax.fori_loop(0, max(n + 6, 16), step, 0)
    back_copy(n - 1).wait()

    lane = lax.broadcasted_iota(jnp.int32, (rows, 128), 1)
    parts = [pl.ds(i * 128, 128) for i in range(vocab // 128)]

    def rows_of(d):
        return pl.ds(pl.multiple_of(d * rows, rows), rows)

    def spread(row):
        return jnp.transpose(jnp.broadcast_to(row, (128, 128)))[:rows]

    def local(h, d, _):
        r = rows_of(d)
        lab = spread(labs[d][:1]) - me * vocab
        cols[r, :] = lab
        m = acc[r, parts[0]]
        for p in parts[1:]:
            m = jnp.maximum(m, acc[r, p])
        m = jnp.max(m, 1, keepdims=True)
        total = right = jnp.zeros((rows, 128), F32)
        for i, p in enumerate(parts):
            z = acc[r, p]
            right += jnp.where(lane + i * 128 == lab, z, 0.0)
            e = jnp.exp(z - m)
            acc[r, p] = e
            total += e
        total, right = jnp.sum(total, 1, keepdims=True), jnp.sum(right, 1, keepdims=True)
        t = jnp.where(lane == 0, m, jnp.where(lane == 1, total, right))
        t = jnp.transpose(jnp.concatenate([t, jnp.zeros((128 - rows, 128), F32)], 0))
        for i in range(3):
            stat[h, i, pl.ds(d - 8 * h, 1), :] = t[i:i + 1]
        scale[h, pl.ds(d - 8 * h, 1), :] = t[:1]
        return 0

    def near_copy(h):
        return _send(s_out.at[h, 0], s_in.at[h, 0], st_send.at[h, 0], st_recv.at[h, 0], pc)

    def far_copy(h, i):
        return _send(s_out.at[h, 1], s_in.at[h, i + 1], st_send.at[h, i + 1], st_recv.at[h, i + 1], far[i])

    def merge(a, b):
        top = jnp.maximum(a[0], b[0])
        return top, a[1] * jnp.exp(a[0] - top) + b[1] * jnp.exp(b[0] - top), a[2] + b[2]

    def figures(ref):
        return ref[0], ref[1], ref[2]

    def start_near(h):
        s_out[h, 0] = stat[h]
        near_copy(h).start()

    def start_far(h):
        near_copy(h).wait()
        for i, a in enumerate(merge(figures(stat.at[h]), figures(s_in.at[h, 0]))):
            s_out[h, 1, i] = a
        for i in range(7):
            far_copy(h, i).start()

    def end_far(h):
        for i in range(7):
            far_copy(h, i).wait()
        a = [figures(s_out.at[h, 1])] + [figures(s_in.at[h, i + 1]) for i in range(7)]
        while len(a) > 1:
            a = [merge(*p) for p in zip(a[::2], a[1::2])]
        lse = jnp.log(a[0][1]) + a[0][0]
        loss_ref[pl.ds(8 * h, 8), :] = lse - a[0][2]
        scale[h] = jnp.exp(scale[h] - lse)

    def g_copy(d):
        return pltpu.make_async_copy(gst.at[rows_of(d)], g_hbm.at[d // 2, d % 2], g_sem.at[d])

    def grad(h, d, _):
        r = rows_of(d)
        f = spread(scale[h, pl.ds(d - 8 * h, 1), :])
        lab = cols[r, :]
        for i, p in enumerate(parts):
            gst[r, p] = (acc[r, p] * f - jnp.where(lane + i * 128 == lab, 1.0, 0.0)).astype(BF16)
        g_copy(d).start()
        return 0

    lax.fori_loop(0, 8, functools.partial(local, 0), 0)
    start_near(0)
    lax.fori_loop(8, 10, functools.partial(local, 1), 0)
    start_far(0)
    lax.fori_loop(10, 16, functools.partial(local, 1), 0)
    start_near(1)
    end_far(0)
    lax.fori_loop(0, 4, functools.partial(grad, 0), 0)
    start_far(1)
    lax.fori_loop(4, 8, functools.partial(grad, 0), 0)
    end_far(1)
    lax.fori_loop(8, 16, functools.partial(grad, 1), 0)
    lax.fori_loop(0, 16, lambda d, _: (g_copy(d).wait(), 0)[1], 0)


def call_gather_logits(x, lab, w, td):
    rows, depth = x.shape
    vocab = w.shape[1]
    s = GATHER_SLOTS
    anywhere, vmem = pl.BlockSpec(memory_space=pl.ANY), pl.BlockSpec(memory_space=pltpu.VMEM)
    return pl.pallas_call(
        functools.partial(gather_logits, td),
        out_shape=(
            jax.ShapeDtypeStruct((8, 2, rows, depth), BF16),
            jax.ShapeDtypeStruct((8, 2, rows, vocab), BF16),
            jax.ShapeDtypeStruct((16, 128), F32),
        ),
        in_specs=[anywhere, vmem, anywhere],
        out_specs=(anywhere, anywhere, vmem),
        scratch_shapes=[
            pltpu.VMEM((s, 8, 2, rows, td), BF16),
            pltpu.VMEM((16 * rows, vocab), F32),
            pltpu.VMEM((2, td, vocab), BF16),
            pltpu.VMEM((16, 8, 128), jnp.int32),
            pltpu.VMEM((16 * rows, 128), jnp.int32),
            pltpu.VMEM((2, 3, 8, 128), F32),
            pltpu.VMEM((2, 8, 128), F32),
            pltpu.VMEM((2, 2, 3, 8, 128), F32),
            pltpu.VMEM((2, 8, 3, 8, 128), F32),
            pltpu.VMEM((16 * rows, vocab), BF16),
            pltpu.SemaphoreType.DMA((10, s)),
            pltpu.SemaphoreType.DMA((10, s)),
            pltpu.SemaphoreType.DMA((s,)),
            pltpu.SemaphoreType.DMA((s,)),
            pltpu.SemaphoreType.DMA((2,)),
            pltpu.SemaphoreType.DMA((4,)),
            pltpu.SemaphoreType.DMA((4,)),
            pltpu.SemaphoreType.DMA((2, 8)),
            pltpu.SemaphoreType.DMA((2, 8)),
            pltpu.SemaphoreType.DMA((16,)),
        ],
        compiler_params=pltpu.CompilerParams(
            collective_id=0, has_side_effects=True, vmem_limit_bytes=67043328),
        cost_estimate=pl.CostEstimate(flops=2 * 16 * rows * depth * vocab, bytes_accessed=depth * vocab * 2, transcendentals=0),
        name="gather_logits",
    )(x, lab, w)


SLOTS = 8


def states_grad(td, early, g_hbm, w_hbm, xf_hbm, out_ref, dw_hbm, gv, wb, xt, dwb, f, s0, r0, s1, r1, s2, r2, s3, r3,
                g_sem, w_sem, x_sem, dw_sem, send, recv):
    me, sx, sy, sz, sc = _where_am_i()
    rows = g_hbm.shape[2]
    depth, vocab = w_hbm.shape
    n = depth // td
    third = rows // 3
    core = me % 2
    px, py, pz, pc = me + sx, me + sy, me + sz, me + sc
    chip = me // 2
    cx, cy, cz = sx // 2, sy // 2, sz // 2

    for h, c in enumerate((core, 1 - core)):
        pltpu.make_async_copy(g_hbm.at[:, c], gv.at[h], g_sem.at[h]).start()

    def w_copy(k):
        rows_k = pl.ds(pl.multiple_of(k * td, td), td)
        return pltpu.make_async_copy(w_hbm.at[rows_k, :], wb.at[k % 2], w_sem.at[k % 2])

    def x_copy(k, h):
        c = core if h == 0 else 1 - core
        cols = pl.ds(pl.multiple_of(k * td, td), td)
        return pltpu.make_async_copy(xf_hbm.at[:, c, :, cols], xt.at[k % 2, h], x_sem.at[k % 2, h])

    def dw_copy(k):
        rows_k = pl.ds(pl.multiple_of(k * td, td), td)
        return pltpu.make_async_copy(dwb.at[k % 2], dw_hbm.at[rows_k, :], dw_sem.at[k % 2])

    w_copy(0).start()
    for h in range(2):
        x_copy(0, h).start()
    _greet((px, py, pz, pc))

    def copies(k):
        s = k % SLOTS

        def copy(i):
            if i == 0:
                src, dst, p = s0.at[s], r0.at[s], pc
            elif i < 4:
                src, dst, p = s1.at[s, pl.ds((i - 1) * third, third)], r1.at[s, i - 1], (pz, px, py)[i - 1]
            elif i < 7:
                src, dst, p = s2.at[s, i - 4], r2.at[s, i - 4], (py, pz, px)[i - 4]
            else:
                src, dst, p = s3.at[s, i - 7], r3.at[s, i - 7], (px, py, pz)[i - 7]
            return _send(src, dst, send.at[i, s], recv.at[i, s], p)

        return copy

    def both(s, dest):
        return f[s, dest] + r0[s, dest].astype(F32)

    for h, c in enumerate((core, 1 - core)):
        pltpu.make_async_copy(g_hbm.at[:, c], gv.at[h], g_sem.at[h]).wait()

    stages = ((1, range(0, 1), range(1, 4)), (2, range(1, 4), range(4, 7)), (4, range(4, 7), range(7, 10)), (6, range(7, 10), ()))

    def receive(lag, k):
        for i in stages[lag][1]:
            copies(k)(i).wait_recv()

    def add(lag, k):
        s = k % SLOTS
        if lag == 0:
            s1[s] = both(s, chip + cx + cy + cz).astype(BF16)
        elif lag == 1:
            for i, dest in enumerate((chip + cx + cy, chip + cy + cz, chip + cz + cx)):
                total = both(s, dest)
                a, b = i * third, (i + 1) * third
                if i > 0:
                    s2[s, i, :a] = total[:a].astype(BF16)
                s2[s, i, a:b] = (total[a:b] + r1[s, i].astype(F32)).astype(BF16)
                if i < 2:
                    s2[s, i, b:] = total[b:].astype(BF16)
        elif lag == 2:
            for i, dest in enumerate((chip + cx, chip + cy, chip + cz)):
                s3[s, i] = (both(s, dest) + r2[s, i].astype(F32)).astype(BF16)
        else:
            total = both(s, chip) + r3[s, 0].astype(F32) + r3[s, 1].astype(F32) + r3[s, 2].astype(F32)
            out_ref[:, pl.ds(pl.multiple_of(k * td, td), td)] = total.astype(BF16)

    def forward(lag, k):
        for i in stages[lag][2]:
            copies(k)(i).start()
        if lag == 3:
            for i in range(10):
                copies(k)(i).wait_send()

    def term(h, t):
        lhs = gv[h].reshape(8 * rows, vocab)
        return lax.dot_general(
            lhs, wb[t % 2], (((1,), (1,)), ((), ())), preferred_element_type=F32).reshape(8, rows, td)

    def fetch(t):
        w_copy(t).wait()

        @pl.when(t + 1 < n)
        def _():
            w_copy(t + 1).start()

    def edge(t, _):
        for lag in range(4):
            k = t - stages[lag][0]

            @pl.when((k >= 0) & (k < n))
            def _():
                receive(lag, k)
                add(lag, k)
                forward(lag, k)

        @pl.when(t < n)
        def _():
            fetch(t)
            s0[t % SLOTS] = term(1, t).astype(BF16)
            copies(t)(0).start()
            f[t % SLOTS] = term(0, t)

        matrix_tile(t)
        return 0

    def steady(t, _):
        fetch(t)
        for lag in range(4):
            receive(lag, t - stages[lag][0])
        for lag in range(4):
            add(lag, t - stages[lag][0])
        for lag in range(4):
            forward(lag, t - stages[lag][0])
        s0[t % SLOTS] = term(1, t).astype(BF16)
        copies(t)(0).start()
        f[t % SLOTS] = term(0, t)
        matrix_tile(t)
        return 0

    def matrix_tile(t):
        ki = jnp.where(t < n, t // 3, n // 3 + t - n)

        @pl.when((ki < early) & ((t % 3 == 2) | (t >= n)))
        def _():
            b = ki % 2
            for h in range(2):
                x_copy(ki, h).wait()

            @pl.when(ki + 1 < early)
            def _():
                for h in range(2):
                    x_copy(ki + 1, h).start()

            @pl.when(ki >= 2)
            def _():
                dw_copy(ki - 2).wait()

            dwb[b] = lax.dot_general(
                xt[b].reshape(16 * rows, td), gv[...].reshape(16 * rows, vocab), (((0,), (0,)), ((), ())),
                preferred_element_type=F32).astype(BF16)
            dw_copy(ki).start()

    lax.fori_loop(0, 6, edge, 0)
    lax.fori_loop(6, n, steady, 0)
    lax.fori_loop(n, n + 6, edge, 0)
    for k in (early - 2, early - 1):
        dw_copy(k).wait()


def call_states_grad(g, w, xf, td, early):
    rows, vocab = g.shape[2:]
    depth = w.shape[0]
    s = SLOTS
    anywhere, vmem = pl.BlockSpec(memory_space=pl.ANY), pl.BlockSpec(memory_space=pltpu.VMEM)
    blocks = lambda *shape, dtype=BF16: pltpu.VMEM((*shape, td), dtype)
    return pl.pallas_call(
        functools.partial(states_grad, td, early),
        out_shape=(jax.ShapeDtypeStruct((rows, depth), BF16), jax.ShapeDtypeStruct((early * td, vocab), BF16)),
        in_specs=[anywhere, anywhere, anywhere],
        out_specs=(vmem, anywhere),
        scratch_shapes=[
            pltpu.VMEM((2, 8, rows, vocab), BF16),
            pltpu.VMEM((2, td, vocab), BF16),
            blocks(2, 2, 8, rows),
            pltpu.VMEM((2, td, vocab), BF16),
            blocks(s, 8, rows, dtype=F32),
            blocks(s, 8, rows),
            blocks(s, 8, rows),
            blocks(s, rows),
            blocks(s, 3, rows // 3),
            blocks(s, 3, rows),
            blocks(s, 3, rows),
            blocks(s, 3, rows),
            blocks(s, 3, rows),
            pltpu.SemaphoreType.DMA((2,)),
            pltpu.SemaphoreType.DMA((2,)),
            pltpu.SemaphoreType.DMA((2, 2)),
            pltpu.SemaphoreType.DMA((2,)),
            pltpu.SemaphoreType.DMA((10, s)),
            pltpu.SemaphoreType.DMA((10, s)),
        ],
        compiler_params=pltpu.CompilerParams(
            collective_id=1, has_side_effects=True, vmem_limit_bytes=67043328),
        cost_estimate=pl.CostEstimate(flops=2 * 16 * rows * depth * vocab, bytes_accessed=depth * vocab * 2, transcendentals=0),
        name="states_grad",
    )(g, w, xf)


def matrix_grad(early, x_ref, g_ref, dw_hbm, out_hbm, made, kept, made_sem, in_sem, kept_sem):
    i, n = pl.program_id(0), pl.num_programs(0)
    tile = x_ref.shape[1]

    def at(k):
        return pl.ds(pl.multiple_of(k * tile, tile), tile)

    def made_out(k):
        return pltpu.make_async_copy(made.at[k % 2], out_hbm.at[at(early + k), :], made_sem.at[k % 2])

    def kept_in(k):
        return pltpu.make_async_copy(dw_hbm.at[at(k), :], kept.at[k % 3], in_sem.at[k % 3])

    def kept_out(k):
        return pltpu.make_async_copy(kept.at[k % 3], out_hbm.at[at(k), :], kept_sem.at[k % 3])

    @pl.when(i == 0)
    def _():
        kept_in(0).start()

    @pl.when(i >= 2)
    def _():
        kept_out(i - 2).wait()
        made_out(i - 2).wait()

    @pl.when(i + 1 < n)
    def _():
        kept_in(i + 1).start()

    kept_in(i).wait()
    kept_out(i).start()
    made[i % 2] = lax.dot_general(
        x_ref[...], g_ref[...], (((0,), (0,)), ((), ())), preferred_element_type=F32).astype(BF16)
    made_out(i).start()

    @pl.when(i == n - 1)
    def _():
        for k in (n - 2, n - 1):
            kept_out(k).wait()
            made_out(k).wait()


def call_matrix_grad(x, g, dw, tile):
    rows, depth = x.shape
    vocab = g.shape[1]
    early = dw.shape[0] // tile
    anywhere = pl.BlockSpec(memory_space=pl.ANY)
    return pl.pallas_call(
        functools.partial(matrix_grad, early),
        grid=(depth // tile - early,),
        out_shape=jax.ShapeDtypeStruct((depth, vocab), BF16),
        in_specs=[pl.BlockSpec((rows, tile), lambda i: (0, early + i)), pl.BlockSpec((rows, vocab), lambda i: (0, 0)), anywhere],
        out_specs=anywhere,
        scratch_shapes=[
            pltpu.VMEM((2, tile, vocab), BF16),
            pltpu.VMEM((3, tile, vocab), BF16),
            pltpu.SemaphoreType.DMA((2,)),
            pltpu.SemaphoreType.DMA((3,)),
            pltpu.SemaphoreType.DMA((3,)),
        ],
        compiler_params=pltpu.CompilerParams(vmem_limit_bytes=60 << 20),
        cost_estimate=pl.CostEstimate(flops=rows * depth * vocab, bytes_accessed=2 * depth * (rows + vocab), transcendentals=0),
        name="matrix_grad",
    )(x, g, dw)


def solution(mesh):
    def step(x, w, label):
        rows, depth = x.shape
        vocab = w.shape[1]
        td = 512 if depth % 512 == 0 and depth > 4096 else 128
        me = lax.axis_index("tp")
        lab = jnp.pad(label[None, :], ((0, 7), (0, 128 - rows)))
        xf, g, loss = call_gather_logits(x, lab, w, td)
        by_x, part = call_states_grad(g, w, xf, td, depth // td // 2)
        by_w = call_matrix_grad(xf.reshape(16 * rows, depth), g.reshape(16 * rows, vocab), part, td)
        return lax.dynamic_slice_in_dim(loss[:, :rows], me, 1)[0], by_x, by_w

    return jax.shard_map(
        step,
        mesh=mesh,
        in_specs=(P(("dp", "tp"), None), P(None, "tp"), P(("dp", "tp"))),
        out_specs=(P(("dp", "tp")), P(("dp", "tp"), None), P("dp", "tp")),
        check_vma=False,
    )
```

```python
import functools

import jax
import jax.numpy as jnp
from jax import lax
from jax.experimental import pallas as pl
from jax.experimental.pallas import tpu as pltpu
from jax.sharding import PartitionSpec as P

MESH = pl.DeviceIdType.MESH
F32, BF16 = jnp.float32, jnp.bfloat16


def _where_am_i():
    me = lax.axis_index("tp")
    x, y, z, c = me // 8, (me // 4) % 2, (me // 2) % 2, me % 2
    return me, 8 - 16 * x, 4 - 8 * y, 2 - 4 * z, 1 - 2 * c


def _greet(peers):
    barrier = pltpu.get_barrier_semaphore()
    for p in peers:
        pl.semaphore_signal(barrier, inc=1, device_id={"tp": p}, device_id_type=MESH)
    pl.semaphore_wait(barrier, len(peers))


def _send(src, dst, send_sem, recv_sem, peer):
    return pltpu.make_async_remote_copy(
        src_ref=src, dst_ref=dst, send_sem=send_sem, recv_sem=recv_sem,
        device_id={"tp": peer}, device_id_type=MESH)


GATHER_SLOTS = 12


def gather_logits(td, x_hbm, lab_ref, w_hbm, xf_hbm, g_hbm, loss_ref,
                  xg, acc, wb, labs, cols, stat, scale, s_out, s_in, gst,
                  send, recv, own_sem, back_sem, w_sem, lab_send, lab_recv, st_send, st_recv, g_sem):
    me, sx, sy, sz, sc = _where_am_i()
    rows, depth = x_hbm.shape
    n = depth // td
    third = rows // 3
    vocab = acc.shape[1]
    core = me % 2
    px, py, pz, pc = me + sx, me + sy, me + sz, me + sc
    far = (px, py, pz, px + sy, py + sz, pz + sx, px + sy + sz)
    _greet((*far, pc))

    def at(k):
        return pl.ds(pl.multiple_of(k * td, td), td)

    def block(k, dev):
        return xg.at[k % GATHER_SLOTS, dev // 2, dev % 2]

    def copies(k):
        s = k % GATHER_SLOTS

        def copy(i):
            if i < 3:
                src, dst, p = x_hbm.at[:, at(k)], block(k, me), (px, py, pz)[i]
            elif i < 6:
                dev, p = ((px, py), (py, pz), (pz, px))[i - 3]
                src = dst = block(k, dev)
            elif i < 9:
                dev, p = ((px + sy, pz), (py + sz, px), (pz + sx, py))[i - 6]
                src = dst = block(k, dev).at[pl.ds((i - 6) * third, third)]
            else:
                p = pc
                src = dst = xg.at[s, :, core]
            return _send(src, dst, send.at[i, s], recv.at[i, s], p)

        return copy

    def own_copy(k):
        return pltpu.make_async_copy(x_hbm.at[:, at(k)], block(k, me), own_sem.at[k % GATHER_SLOTS])

    def back_copy(k):
        s = k % GATHER_SLOTS
        return pltpu.make_async_copy(xg.at[s], xf_hbm.at[:, :, :, at(k)], back_sem.at[s])

    def w_copy(k):
        rows_k = pl.ds(pl.multiple_of(k * td, td), td)
        return pltpu.make_async_copy(w_hbm.at[rows_k, :], wb.at[k % 2], w_sem.at[k % 2])

    labs[me, :1, :rows] = lab_ref[...]

    def lab_copy(i):
        size = 1 << i
        p = (pc, pz, py, px)[i]
        part = labs.at[pl.ds((me // size) * size, size)]
        return _send(part, part, lab_send.at[i], lab_recv.at[i], p)

    w_copy(0).start()

    def step(t, _):
        for i in range(5):
            @pl.when(t == 3 * i + 2)
            def _():
                if i > 0:
                    lab_copy(i - 1).wait()
                if i < 4:
                    lab_copy(i).start()

        k4 = t - 4

        @pl.when((k4 >= 0) & (k4 < n))
        def _():
            cs = copies(k4)
            for i in range(6, 9):
                cs(i).wait_recv()
            own_copy(k4).wait()
            cs(9).start()

        k3 = t - 3

        @pl.when((k3 >= 0) & (k3 < n))
        def _():
            cs = copies(k3)
            for i in range(3, 6):
                cs(i).wait_recv()
            for i in range(6, 9):
                cs(i).start()

        k2 = t - 2

        @pl.when((k2 >= 0) & (k2 < n))
        def _():
            cs = copies(k2)
            for i in range(3):
                cs(i).wait_recv()
            for i in range(3, 6):
                cs(i).start()

        @pl.when(t < n)
        def _():
            cs = copies(t)
            for i in range(3):
                cs(i).start()
            own_copy(t).start()

        @pl.when(t == 1)
        def _():
            acc[...] = jnp.zeros_like(acc)

        k5 = t - 5

        @pl.when((k5 >= 0) & (k5 < n))
        def _():
            cs = copies(k5)
            cs(9).wait_recv()
            w_copy(k5).wait()

            @pl.when(k5 + 1 < n)
            def _():
                w_copy(k5 + 1).start()

            @pl.when(k5 > 0)
            def _():
                back_copy(k5 - 1).wait()

            back_copy(k5).start()
            for i in range(10):
                cs(i).wait_send()
            lhs = xg[k5 % GATHER_SLOTS].reshape(16 * rows, td)
            acc[...] += jnp.dot(lhs, wb[k5 % 2], preferred_element_type=F32)

        return 0

    lax.fori_loop(0, max(n + 5, 16), step, 0)
    back_copy(n - 1).wait()

    lane = lax.broadcasted_iota(jnp.int32, (rows, 128), 1)
    parts = [pl.ds(i * 128, 128) for i in range(vocab // 128)]

    def rows_of(d):
        return pl.ds(pl.multiple_of(d * rows, rows), rows)

    def spread(row):
        return jnp.transpose(jnp.broadcast_to(row, (128, 128)))[:rows]

    def local(h, pair, _):
        ds = (2 * pair, 2 * pair + 1)
        labels, tops, sums = [], [], []
        for d in ds:
            labels.append(spread(labs[d][:1]) - me * vocab)
            m = acc[rows_of(d), parts[0]]
            for p in parts[1:]:
                m = jnp.maximum(m, acc[rows_of(d), p])
            tops.append(jnp.max(m, 1, keepdims=True))
        for d, lab, m in zip(ds, labels, tops):
            cols[rows_of(d), :] = lab
            total = right = jnp.zeros((rows, 128), F32)
            for i, p in enumerate(parts):
                z = acc[rows_of(d), p]
                right += jnp.where(lane + i * 128 == lab, z, 0.0)
                e = jnp.exp(z - m)
                acc[rows_of(d), p] = e
                total += e
            sums.append((total, right))
        for d, m, (total, right) in zip(ds, tops, sums):
            total, right = jnp.sum(total, 1, keepdims=True), jnp.sum(right, 1, keepdims=True)
            t = jnp.where(lane == 0, m, jnp.where(lane == 1, total, right))
            t = jnp.transpose(jnp.concatenate([t, jnp.zeros((128 - rows, 128), F32)], 0))
            for i in range(3):
                stat[h, i, pl.ds(d - 8 * h, 1), :] = t[i:i + 1]
            scale[h, pl.ds(d - 8 * h, 1), :] = t[:1]
        return 0

    def near_copy(h):
        return _send(s_out.at[h, 0], s_in.at[h, 0], st_send.at[h, 0], st_recv.at[h, 0], pc)

    def far_copy(h, i):
        return _send(s_out.at[h, 1], s_in.at[h, i + 1], st_send.at[h, i + 1], st_recv.at[h, i + 1], far[i])

    def merge(a, b):
        top = jnp.maximum(a[0], b[0])
        return top, a[1] * jnp.exp(a[0] - top) + b[1] * jnp.exp(b[0] - top), a[2] + b[2]

    def figures(ref):
        return ref[0], ref[1], ref[2]

    def start_near(h):
        s_out[h, 0] = stat[h]
        near_copy(h).start()

    def start_far(h):
        near_copy(h).wait()
        for i, a in enumerate(merge(figures(stat.at[h]), figures(s_in.at[h, 0]))):
            s_out[h, 1, i] = a
        for i in range(7):
            far_copy(h, i).start()

    def end_far(h):
        for i in range(7):
            far_copy(h, i).wait()
        a = [figures(s_out.at[h, 1])] + [figures(s_in.at[h, i + 1]) for i in range(7)]
        while len(a) > 1:
            a = [merge(*p) for p in zip(a[::2], a[1::2])]
        lse = jnp.log(a[0][1]) + a[0][0]
        loss_ref[pl.ds(8 * h, 8), :] = lse - a[0][2]
        scale[h] = jnp.exp(scale[h] - lse)

    def g_copy(d):
        return pltpu.make_async_copy(gst.at[rows_of(d)], g_hbm.at[d // 2, d % 2], g_sem.at[d])

    def grad(h, pair, _):
        ds = (2 * pair, 2 * pair + 1)
        factors = [spread(scale[h, pl.ds(d - 8 * h, 1), :]) for d in ds]
        for d, f in zip(ds, factors):
            lab = cols[rows_of(d), :]
            for i, p in enumerate(parts):
                g = acc[rows_of(d), p] * f - jnp.where(lane + i * 128 == lab, 1.0, 0.0)
                gst[rows_of(d), p] = g.astype(BF16)
            g_copy(d).start()
        return 0

    lax.fori_loop(0, 4, functools.partial(local, 0), 0)
    start_near(0)
    lax.fori_loop(4, 5, functools.partial(local, 1), 0)
    start_far(0)
    lax.fori_loop(5, 8, functools.partial(local, 1), 0)
    start_near(1)
    end_far(0)
    lax.fori_loop(0, 2, functools.partial(grad, 0), 0)
    start_far(1)
    lax.fori_loop(2, 4, functools.partial(grad, 0), 0)
    end_far(1)
    lax.fori_loop(4, 8, functools.partial(grad, 1), 0)
    lax.fori_loop(0, 16, lambda d, _: (g_copy(d).wait(), 0)[1], 0)


def call_gather_logits(x, lab, w, td):
    rows, depth = x.shape
    vocab = w.shape[1]
    s = GATHER_SLOTS
    anywhere, vmem = pl.BlockSpec(memory_space=pl.ANY), pl.BlockSpec(memory_space=pltpu.VMEM)
    return pl.pallas_call(
        functools.partial(gather_logits, td),
        out_shape=(
            jax.ShapeDtypeStruct((8, 2, rows, depth), BF16),
            jax.ShapeDtypeStruct((8, 2, rows, vocab), BF16),
            jax.ShapeDtypeStruct((16, 128), F32),
        ),
        in_specs=[anywhere, vmem, anywhere],
        out_specs=(anywhere, anywhere, vmem),
        scratch_shapes=[
            pltpu.VMEM((s, 8, 2, rows, td), BF16),
            pltpu.VMEM((16 * rows, vocab), F32),
            pltpu.VMEM((2, td, vocab), BF16),
            pltpu.VMEM((16, 8, 128), jnp.int32),
            pltpu.VMEM((16 * rows, 128), jnp.int32),
            pltpu.VMEM((2, 3, 8, 128), F32),
            pltpu.VMEM((2, 8, 128), F32),
            pltpu.VMEM((2, 2, 3, 8, 128), F32),
            pltpu.VMEM((2, 8, 3, 8, 128), F32),
            pltpu.VMEM((16 * rows, vocab), BF16),
            pltpu.SemaphoreType.DMA((10, s)),
            pltpu.SemaphoreType.DMA((10, s)),
            pltpu.SemaphoreType.DMA((s,)),
            pltpu.SemaphoreType.DMA((s,)),
            pltpu.SemaphoreType.DMA((2,)),
            pltpu.SemaphoreType.DMA((4,)),
            pltpu.SemaphoreType.DMA((4,)),
            pltpu.SemaphoreType.DMA((2, 8)),
            pltpu.SemaphoreType.DMA((2, 8)),
            pltpu.SemaphoreType.DMA((16,)),
        ],
        compiler_params=pltpu.CompilerParams(
            collective_id=0, has_side_effects=True, vmem_limit_bytes=67043328),
        cost_estimate=pl.CostEstimate(flops=2 * 16 * rows * depth * vocab, bytes_accessed=depth * vocab * 2, transcendentals=0),
        name="gather_logits",
    )(x, lab, w)


SLOTS = 8


def states_grad(td, early, g_hbm, w_hbm, xf_hbm, out_ref, dw_hbm, gv, wb, xt, dwb, f, s0, r0, s1, r1, s2, r2, s3, r3,
                g_sem, w_sem, x_sem, dw_sem, send, recv):
    me, sx, sy, sz, sc = _where_am_i()
    rows = g_hbm.shape[2]
    depth, vocab = w_hbm.shape
    n = depth // td
    third = rows // 3
    core = me % 2
    px, py, pz, pc = me + sx, me + sy, me + sz, me + sc
    chip = me // 2
    cx, cy, cz = sx // 2, sy // 2, sz // 2

    def g_copy(h):
        return pltpu.make_async_copy(g_hbm.at[:, core if h == 0 else 1 - core], gv.at[h], g_sem.at[h])

    g_copy(1).start()

    def w_copy(k):
        rows_k = pl.ds(pl.multiple_of(k * td, td), td)
        return pltpu.make_async_copy(w_hbm.at[rows_k, :], wb.at[k % 2], w_sem.at[k % 2])

    def x_copy(k, h):
        c = core if h == 0 else 1 - core
        cols = pl.ds(pl.multiple_of(k * td, td), td)
        return pltpu.make_async_copy(xf_hbm.at[:, c, :, cols], xt.at[k % 2, h], x_sem.at[k % 2, h])

    def dw_copy(k):
        rows_k = pl.ds(pl.multiple_of(k * td, td), td)
        return pltpu.make_async_copy(dwb.at[k % 2], dw_hbm.at[rows_k, :], dw_sem.at[k % 2])

    w_copy(0).start()
    g_copy(0).start()
    for h in range(2):
        x_copy(0, h).start()
    _greet((px, py, pz, pc))

    def copies(k):
        s = k % SLOTS

        def copy(i):
            if i == 0:
                src, dst, p = s0.at[s], r0.at[s], pc
            elif i < 4:
                src, dst, p = s1.at[s, pl.ds((i - 1) * third, third)], r1.at[s, i - 1], (pz, px, py)[i - 1]
            elif i < 7:
                src, dst, p = s2.at[s, i - 4], r2.at[s, i - 4], (py, pz, px)[i - 4]
            else:
                src, dst, p = s3.at[s, i - 7], r3.at[s, i - 7], (px, py, pz)[i - 7]
            return _send(src, dst, send.at[i, s], recv.at[i, s], p)

        return copy

    def both(s, dest):
        return f[s, dest] + r0[s, dest].astype(F32)

    g_copy(1).wait()

    stages = ((1, range(0, 1), range(1, 4)), (2, range(1, 4), range(4, 7)), (4, range(4, 7), range(7, 10)), (6, range(7, 10), ()))

    def receive(lag, k):
        for i in stages[lag][1]:
            copies(k)(i).wait_recv()

    def add(lag, k):
        s = k % SLOTS
        if lag == 0:
            s1[s] = both(s, chip + cx + cy + cz).astype(BF16)
        elif lag == 1:
            for i, dest in enumerate((chip + cx + cy, chip + cy + cz, chip + cz + cx)):
                total = both(s, dest)
                a, b = i * third, (i + 1) * third
                if i > 0:
                    s2[s, i, :a] = total[:a].astype(BF16)
                s2[s, i, a:b] = (total[a:b] + r1[s, i].astype(F32)).astype(BF16)
                if i < 2:
                    s2[s, i, b:] = total[b:].astype(BF16)
        elif lag == 2:
            for i, dest in enumerate((chip + cx, chip + cy, chip + cz)):
                s3[s, i] = (both(s, dest) + r2[s, i].astype(F32)).astype(BF16)
        else:
            total = both(s, chip) + r3[s, 0].astype(F32) + r3[s, 1].astype(F32) + r3[s, 2].astype(F32)
            out_ref[:, pl.ds(pl.multiple_of(k * td, td), td)] = total.astype(BF16)

    def forward(lag, k):
        for i in stages[lag][2]:
            copies(k)(i).start()
        if lag == 3:
            for i in range(10):
                copies(k)(i).wait_send()

    def term(h, t):
        lhs = gv[h].reshape(8 * rows, vocab)
        return lax.dot_general(
            lhs, wb[t % 2], (((1,), (1,)), ((), ())), preferred_element_type=F32).reshape(8, rows, td)

    def fetch(t):
        w_copy(t).wait()

        @pl.when(t + 1 < n)
        def _():
            w_copy(t + 1).start()

    def edge(t, _):
        for lag in range(4):
            k = t - stages[lag][0]

            @pl.when((k >= 0) & (k < n))
            def _():
                receive(lag, k)
                add(lag, k)
                forward(lag, k)

        @pl.when(t < n)
        def _():
            fetch(t)
            s0[t % SLOTS] = term(1, t).astype(BF16)
            copies(t)(0).start()

            @pl.when(t == 0)
            def _():
                g_copy(0).wait()

            f[t % SLOTS] = term(0, t)

        matrix_tile(t)
        return 0

    def steady(t, _):
        fetch(t)
        for lag in range(4):
            receive(lag, t - stages[lag][0])
        for lag in range(4):
            add(lag, t - stages[lag][0])
        for lag in range(4):
            forward(lag, t - stages[lag][0])
        s0[t % SLOTS] = term(1, t).astype(BF16)
        copies(t)(0).start()
        f[t % SLOTS] = term(0, t)
        matrix_tile(t)
        return 0

    def matrix_tile(t):
        ki = jnp.where(t < n, t // 3, n // 3 + t - n)

        @pl.when((ki < early) & ((t % 3 == 2) | (t >= n)))
        def _():
            b = ki % 2
            for h in range(2):
                x_copy(ki, h).wait()

            @pl.when(ki + 1 < early)
            def _():
                for h in range(2):
                    x_copy(ki + 1, h).start()

            @pl.when(ki >= 2)
            def _():
                dw_copy(ki - 2).wait()

            dwb[b] = lax.dot_general(
                xt[b].reshape(16 * rows, td), gv[...].reshape(16 * rows, vocab), (((0,), (0,)), ((), ())),
                preferred_element_type=F32).astype(BF16)
            dw_copy(ki).start()

    lax.fori_loop(0, 6, edge, 0)
    lax.fori_loop(6, n, steady, 0)
    lax.fori_loop(n, n + 6, edge, 0)
    for k in (early - 2, early - 1):
        dw_copy(k).wait()


def call_states_grad(g, w, xf, td, early):
    rows, vocab = g.shape[2:]
    depth = w.shape[0]
    s = SLOTS
    anywhere, vmem = pl.BlockSpec(memory_space=pl.ANY), pl.BlockSpec(memory_space=pltpu.VMEM)
    blocks = lambda *shape, dtype=BF16: pltpu.VMEM((*shape, td), dtype)
    return pl.pallas_call(
        functools.partial(states_grad, td, early),
        out_shape=(jax.ShapeDtypeStruct((rows, depth), BF16), jax.ShapeDtypeStruct((early * td, vocab), BF16)),
        in_specs=[anywhere, anywhere, anywhere],
        out_specs=(vmem, anywhere),
        scratch_shapes=[
            pltpu.VMEM((2, 8, rows, vocab), BF16),
            pltpu.VMEM((2, td, vocab), BF16),
            blocks(2, 2, 8, rows),
            pltpu.VMEM((2, td, vocab), BF16),
            blocks(s, 8, rows, dtype=F32),
            blocks(s, 8, rows),
            blocks(s, 8, rows),
            blocks(s, rows),
            blocks(s, 3, rows // 3),
            blocks(s, 3, rows),
            blocks(s, 3, rows),
            blocks(s, 3, rows),
            blocks(s, 3, rows),
            pltpu.SemaphoreType.DMA((2,)),
            pltpu.SemaphoreType.DMA((2,)),
            pltpu.SemaphoreType.DMA((2, 2)),
            pltpu.SemaphoreType.DMA((2,)),
            pltpu.SemaphoreType.DMA((10, s)),
            pltpu.SemaphoreType.DMA((10, s)),
        ],
        compiler_params=pltpu.CompilerParams(
            collective_id=1, has_side_effects=True, vmem_limit_bytes=67043328),
        cost_estimate=pl.CostEstimate(flops=2 * 16 * rows * depth * vocab, bytes_accessed=depth * vocab * 2, transcendentals=0),
        name="states_grad",
    )(g, w, xf)


def matrix_grad(early, x_ref, g_ref, dw_hbm, out_hbm, made, kept, made_sem, in_sem, kept_sem):
    i, n = pl.program_id(0), pl.num_programs(0)
    tile = x_ref.shape[1]

    def at(k):
        return pl.ds(pl.multiple_of(k * tile, tile), tile)

    def made_out(k):
        return pltpu.make_async_copy(made.at[k % 2], out_hbm.at[at(early + k), :], made_sem.at[k % 2])

    def kept_in(k):
        return pltpu.make_async_copy(dw_hbm.at[at(k), :], kept.at[k % 3], in_sem.at[k % 3])

    def kept_out(k):
        return pltpu.make_async_copy(kept.at[k % 3], out_hbm.at[at(k), :], kept_sem.at[k % 3])

    @pl.when(i == 0)
    def _():
        kept_in(0).start()

    @pl.when(i >= 2)
    def _():
        kept_out(i - 2).wait()
        made_out(i - 2).wait()

    @pl.when(i + 1 < n)
    def _():
        kept_in(i + 1).start()

    kept_in(i).wait()
    kept_out(i).start()
    made[i % 2] = lax.dot_general(
        x_ref[...], g_ref[...], (((0,), (0,)), ((), ())), preferred_element_type=F32).astype(BF16)
    made_out(i).start()

    @pl.when(i == n - 1)
    def _():
        for k in (n - 2, n - 1):
            kept_out(k).wait()
            made_out(k).wait()


def call_matrix_grad(x, g, dw, tile):
    rows, depth = x.shape
    vocab = g.shape[1]
    early = dw.shape[0] // tile
    anywhere = pl.BlockSpec(memory_space=pl.ANY)
    return pl.pallas_call(
        functools.partial(matrix_grad, early),
        grid=(depth // tile - early,),
        out_shape=jax.ShapeDtypeStruct((depth, vocab), BF16),
        in_specs=[pl.BlockSpec((rows, tile), lambda i: (0, early + i)), pl.BlockSpec((rows, vocab), lambda i: (0, 0)), anywhere],
        out_specs=anywhere,
        scratch_shapes=[
            pltpu.VMEM((2, tile, vocab), BF16),
            pltpu.VMEM((3, tile, vocab), BF16),
            pltpu.SemaphoreType.DMA((2,)),
            pltpu.SemaphoreType.DMA((3,)),
            pltpu.SemaphoreType.DMA((3,)),
        ],
        compiler_params=pltpu.CompilerParams(vmem_limit_bytes=60 << 20),
        cost_estimate=pl.CostEstimate(flops=rows * depth * vocab, bytes_accessed=2 * depth * (rows + vocab), transcendentals=0),
        name="matrix_grad",
    )(x, g, dw)


def solution(mesh):
    def step(x, w, label):
        rows, depth = x.shape
        vocab = w.shape[1]
        td = 512 if depth % 512 == 0 and depth > 4096 else 128
        me = lax.axis_index("tp")
        lab = label.reshape(1, rows)
        xf, g, loss = call_gather_logits(x, lab, w, td)
        by_x, part = call_states_grad(g, w, xf, td, depth // td // 2)
        by_w = call_matrix_grad(xf.reshape(16 * rows, depth), g.reshape(16 * rows, vocab), part, td)
        return lax.dynamic_slice_in_dim(loss[:, :rows], me, 1)[0], by_x, by_w

    return jax.shard_map(
        step,
        mesh=mesh,
        in_specs=(P(("dp", "tp"), None), P(None, "tp"), P(("dp", "tp"))),
        out_specs=(P(("dp", "tp")), P(("dp", "tp"), None), P("dp", "tp")),
        check_vma=False,
    )
```
